32 devices in a mesh: grp: 4 (over z), pair: 8 (over y, x, core).
Axes of the slice: x: 2, y: 2, z: 4, core: 2. Of those that a mesh axis runs over, the one named last changes fastest.
Arguments:
- amplitudes: bfloat16 [64, 512, 512], P('pair', 'grp'), may hold values from -6 to 6
- cholesky: bfloat16 [512, 512, 2048], P('pair', 'grp'), may hold values from -0.09375 to 0.09375
Outputs:
- ladder_term: float32 [512, 4, 64], P('pair', None, 'grp')
The draws below stay inside these ranges and needn't reach their ends.
All inputs are finite; a program needn't handle non-finite values.
Results may differ from the reference program's by a relative error of at most 0.003.
Values may be sent and summed in bfloat16 or wider, within the bound.
A program may use at most 128 MiB of HBM per device.

```python
import jax
import jax.numpy as jnp
from jax import lax

VIRT = 512
NAUX = 2048
A_WIN = 4
NPAIR = 64


def levels(own_key, shape, shards, low, high):
    loudness = 1.0
    for axis_at, shards_of in shards:
        draws = jax.random.uniform(jax.random.fold_in(jax.random.fold_in(own_key, 6), axis_at), (shards_of,), jnp.float32, low / len(shards), high / len(shards))
        loudness = loudness * jnp.repeat(jnp.exp(draws), shape[axis_at] // shards_of).reshape((-1,) + (1,) * (len(shape) - 1 - axis_at))
    return loudness


def bell_draw(own_key, dims, spread, bound, split=(), kind=jnp.bfloat16):
    entries = jax.random.normal(own_key, dims, jnp.float32) * spread
    if len(split) > 0:
        entries = levels(own_key, dims, split, -0.22, 0.18) * entries
    return jnp.clip(entries, min=-bound, max=bound).astype(kind)


def setup_inputs(seed: int = 0) -> dict:
    splits = jax.random.split(jax.random.key(seed), 3)
    amplitudes = bell_draw(splits[0], (NPAIR, VIRT, VIRT), 1.0, 6.0, ((0, 8), (1, 4)))
    cholesky = bell_draw(splits[1], (VIRT, VIRT, NAUX), ((VIRT * VIRT * NAUX) ** -0.25), 0.09375, ((0, 8), (1, 4)))
    return {"amplitudes": amplitudes, "cholesky": cholesky}


def reference(amplitudes, cholesky):
    tiles_count = 8
    tile_width = VIRT // tiles_count
    window_chol = cholesky[:A_WIN]
    flat_chol = cholesky.reshape(VIRT * VIRT, NAUX)

    def one_tile(running, tile_index):
        offset = (tile_index * tile_width).astype(jnp.int32)
        portion = lax.dynamic_slice_in_dim(window_chol, offset, tile_width, 1)
        product = lax.dot_general(flat_chol, portion.reshape(A_WIN * tile_width, NAUX), (((1,), (1,)), ((), ())), preferred_element_type=jnp.float32)
        integrals = product.astype(jnp.bfloat16).reshape(VIRT, VIRT, A_WIN, tile_width)
        amp_slice = lax.dynamic_slice_in_dim(amplitudes, offset, tile_width, 2)
        contrib = lax.dot_general(integrals, amp_slice, (((1, 3), (1, 2)), ((), ())), preferred_element_type=jnp.float32)
        return running + contrib, None

    initial = jnp.zeros((VIRT, A_WIN, NPAIR), jnp.float32)
    result, unused = lax.scan(one_tile, initial, jnp.arange(tiles_count, dtype=jnp.int32))
    return result
```

```python
import functools
import math

import jax
import jax.numpy as jnp
from jax import lax
from jax.experimental import pallas as pl
from jax.experimental.pallas import tpu as pltpu
from jax.sharding import PartitionSpec as P

A_WIN = 4
CORES = 2
ROWS = 512
LANES = 128


def remote(src, dst, send, recv, where):
    return pltpu.make_async_remote_copy(
        src_ref=src, dst_ref=dst, send_sem=send, recv_sem=recv,
        device_id=where, device_id_type=pl.DeviceIdType.MESH,
    )


def build_kernel(groups, pairs, depth, chol, out, wbuf, lbuf, scr, obuf, lsem, osem, hsem,
                 sc_send, sc_recv, z_send, z_recv, pl_send, pl_recv, cc_send, cc_recv):
    g = lax.axis_index("grp")
    p = lax.axis_index("pair")
    chips = pairs // CORES
    core = lax.rem(p, CORES)
    chip = p // CORES
    mate = p + 1 - 2 * core
    brows, dcount, naux = chol.shape
    piece = dcount // pairs
    blocks = dcount // depth
    total = groups * blocks

    def part(tile, who):
        return wbuf.at[tile, :, pl.ds(pl.multiple_of(who * piece, piece), piece), :]

    def fetch(step, slot):
        at = pl.multiple_of(lax.rem(step, blocks) * depth, depth)
        return pltpu.make_async_copy(chol.at[:, pl.ds(at, depth), :], lbuf.at[slot], lsem.at[slot])

    barrier = pltpu.get_barrier_semaphore()
    for j in range(1, pairs):
        pl.semaphore_signal(barrier, inc=1, device_id={"pair": lax.rem(p + j, pairs)}, device_id_type=pl.DeviceIdType.MESH)
    for j in range(1, groups):
        pl.semaphore_signal(barrier, inc=1, device_id={"grp": lax.rem(g + j, groups)}, device_id_type=pl.DeviceIdType.MESH)
    pl.semaphore_wait(barrier, pairs + groups - 2)

    def scatter(who):
        return remote(chol.at[:A_WIN, who * piece:(who + 1) * piece, :], wbuf.at[g, :, who * piece:(who + 1) * piece, :],
                      sc_send.at[who], sc_recv, {"pair": who})

    @pl.when(p == 0)
    def _():
        for who in list(range(CORES, pairs)) + list(range(1, CORES)):
            scatter(who).start()
        own = pltpu.make_async_copy(chol.at[:A_WIN, :piece, :], wbuf.at[g, :, :piece, :], hsem)
        own.start()
        own.wait()

    @pl.when(p != 0)
    def _():
        remote(part(g, p), part(g, p), sc_send.at[0], sc_recv, {"pair": mate}).wait_recv()

    fetch(0, 0).start()

    def along(j):
        to = lax.rem(g + j, groups)
        return remote(part(g, p), part(g, p), z_send.at[j], z_recv.at[g], {"grp": to})

    def plane(tile, j):
        to = lax.rem(p + CORES * j, pairs)
        return remote(part(tile, p), part(tile, p), pl_send.at[tile, j], pl_recv.at[tile, chip], {"pair": to})

    def plane_in(tile, j):
        source = lax.rem(p + CORES * j, pairs)
        return remote(part(tile, source), part(tile, source), pl_send.at[tile, j],
                      pl_recv.at[tile, source // CORES], {"pair": mate})

    def across(tile, j):
        source = lax.rem(p + CORES * j, pairs)
        return remote(part(tile, source), part(tile, source), cc_send.at[tile, j],
                      cc_recv.at[tile, source // CORES], {"pair": mate})

    def across_in(tile, j):
        source = lax.rem(mate + CORES * j, pairs)
        return remote(part(tile, source), part(tile, source), cc_send.at[tile, j],
                      cc_recv.at[tile, source // CORES], {"pair": mate})

    def spread(tile):
        for j in range(1, chips):
            plane(tile, j).start()
        across(tile, 0).start()

    def forward(tile):
        for j in range(1, chips):
            plane_in(tile, j).wait_recv()
            across(tile, j).start()

    def arrive(tile):
        for j in range(chips):
            across_in(tile, j).wait_recv()

    spread(g)
    for j in range(1, groups):
        along(j).start()
    forward(g)
    arrive(g)

    width = dcount
    group = ROWS // depth

    def put(tile, block, slot):
        at = pl.multiple_of(block * depth, depth)
        return pltpu.make_async_copy(obuf.at[slot], out.at[tile, pl.ds(at, depth)], osem.at[slot])

    for k in range(groups):
        tile = lax.rem(g + k, groups)
        nxt = lax.rem(g + k + 1, groups)
        last = k == groups - 1
        if k > 0:
            arrive(tile)

        def step(block, carry, k=k, tile=tile, nxt=nxt, last=last):
            s = k * blocks + block
            slot = lax.rem(s, 2)
            if not last:
                @pl.when(block == 0)
                def _():
                    remote(part(nxt, p), part(nxt, p), z_send.at[0], z_recv.at[nxt], {"pair": mate}).wait_recv()
                    spread(nxt)

                @pl.when(block == blocks // 2 + 1)
                def _():
                    forward(nxt)

            @pl.when(s + 1 < total)
            def _():
                fetch(s + 1, 1 - slot).start()

            fetch(s, slot).wait()

            @pl.when(s >= 2)
            def _():
                put(tile, block, slot).wait()

            weights = wbuf[tile].reshape(A_WIN * width, naux)
            for part_at in range(brows // group):
                b0 = part_at * group
                rows = lbuf[slot, b0:b0 + group].reshape(group * depth, naux)
                product = lax.dot_general(rows, weights, (((1,), (1,)), ((), ())), preferred_element_type=jnp.float32)
                for n in range(scr.shape[1]):
                    scr[part_at, n] = product[:, n * LANES:(n + 1) * LANES]
                for d in range(depth):
                    for n in range(scr.shape[1]):
                        got = scr[part_at, n, pl.ds(d, group, stride=depth), :].astype(jnp.bfloat16)
                        for off in range(0, LANES, width):
                            obuf[slot, d, (n * LANES + off) // width, b0:b0 + group, :] = got[:, off:off + width]
            put(tile, block, slot).start()
            return carry

        lax.fori_loop(0, blocks, step, 0)

    for s in (total - 2, total - 1):
        put(g, 0, s % 2).wait()

    @pl.when(p == 0)
    def _():
        for who in range(1, pairs):
            scatter(who).wait_send()
    for j in range(1, groups):
        along(j).wait_send()
    for k in range(groups):
        tile = lax.rem(g + k, groups)
        for j in range(chips):
            if j > 0:
                plane(tile, j).wait_send()
            across(tile, j).wait_send()


def build(cholesky, groups, pairs):
    brows, dcount, naux = cholesky.shape
    depth = min(16, dcount)
    chips = pairs // CORES
    width = dcount
    out = jax.ShapeDtypeStruct((groups, dcount, A_WIN, brows, width), jnp.bfloat16)
    dma = pltpu.SemaphoreType.DMA
    return pl.pallas_call(
        functools.partial(build_kernel, groups, pairs, depth),
        out_shape=out,
        in_specs=[pl.BlockSpec(memory_space=pl.ANY)],
        out_specs=pl.BlockSpec(memory_space=pl.ANY),
        scratch_shapes=[
            pltpu.VMEM((groups, A_WIN, width, naux), jnp.bfloat16),
            pltpu.VMEM((2, brows, depth, naux), jnp.bfloat16),
            pltpu.VMEM((brows * depth // ROWS, A_WIN * width // LANES, ROWS, LANES), jnp.float32),
            pltpu.VMEM((2, depth, A_WIN, brows, width), jnp.bfloat16),
            dma((2,)), dma((2,)), dma(()),
            dma((pairs,)), dma(()), dma((groups,)), dma((groups,)),
            dma((groups, chips)), dma((groups, chips)), dma((groups, chips)), dma((groups, chips)),
        ],
        compiler_params=pltpu.CompilerParams(collective_id=0, has_side_effects=True, vmem_limit_bytes=60 * 2**20),
        cost_estimate=pl.CostEstimate(
            flops=2 * brows * dcount * A_WIN * width * groups * naux,
            bytes_accessed=cholesky.size * 2 * groups + math.prod(out.shape) * 2, transcendentals=0),
        name="build",
    )(cholesky)


def ladder_kernel(groups, ints, amps, out, acc, flip, got, send, recv):
    g = lax.axis_index("grp")
    i = pl.program_id(0)
    own = flip.shape[0] // groups
    barrier = pltpu.get_barrier_semaphore()

    def ship(j):
        to = lax.rem(g + j, groups)
        return remote(flip.at[pl.ds(pl.multiple_of(to * own, own), own), :], got.at[j],
                      send.at[j], recv.at[j], {"grp": to})

    @pl.when(i == 0)
    def _():
        for j in range(1, groups):
            pl.semaphore_signal(barrier, inc=1, device_id={"grp": lax.rem(g + j, groups)}, device_id_type=pl.DeviceIdType.MESH)
        pl.semaphore_wait(barrier, groups - 1)
        acc[...] = jnp.zeros_like(acc)

    total = acc[...]
    for d in range(ints.shape[1]):
        left = jnp.concatenate([ints[t, d].reshape(acc.shape[0], ints.shape[4]) for t in range(groups)], axis=1)
        right = amps[:, d].reshape(acc.shape[1], amps.shape[3])
        total = total + lax.dot_general(left, right, (((1,), (1,)), ((), ())), preferred_element_type=jnp.float32)
    acc[...] = total

    @pl.when(i == pl.num_programs(0) - 1)
    def _():
        flip[...] = acc[...].T
        for j in range(1, groups):
            ship(j).start()
        mine = flip[pl.ds(pl.multiple_of(g * own, own), own), :]
        for j in range(1, groups):
            ship(j).wait_recv()
            mine = mine + got[j]
        out[...] = mine
        for j in range(1, groups):
            ship(j).wait_send()


def ladder(ints, amps, groups):
    pairs, dcount, each, virt = amps.shape
    brows, width = ints.shape[3:]
    block = min(8, dcount)
    pair_count = pairs * each
    rows = A_WIN * brows
    return pl.pallas_call(
        functools.partial(ladder_kernel, groups),
        out_shape=jax.ShapeDtypeStruct((pair_count // groups, rows), jnp.float32),
        grid=(dcount // block,),
        in_specs=[
            pl.BlockSpec((groups, block, A_WIN, brows, width), lambda i: (0, i, 0, 0, 0)),
            pl.BlockSpec((pairs, block, each, virt), lambda i: (0, i, 0, 0)),
        ],
        out_specs=pl.BlockSpec((pair_count // groups, rows), lambda i: (0, 0)),
        scratch_shapes=[
            pltpu.VMEM((rows, pair_count), jnp.float32),
            pltpu.VMEM((pair_count, rows), jnp.float32),
            pltpu.VMEM((groups, pair_count // groups, rows), jnp.float32),
            pltpu.SemaphoreType.DMA((groups,)),
            pltpu.SemaphoreType.DMA((groups,)),
        ],
        compiler_params=pltpu.CompilerParams(collective_id=1, has_side_effects=True, vmem_limit_bytes=48 * 2**20),
        cost_estimate=pl.CostEstimate(flops=2 * ints.size * pair_count, bytes_accessed=ints.size * 2 + amps.size * 2, transcendentals=0),
        name="ladder",
    )(ints, amps)


def per_device(groups, pairs, amplitudes, cholesky):
    brows = cholesky.shape[0]
    everyone = lax.all_gather(jnp.transpose(amplitudes, (1, 0, 2)), "pair", axis=0)
    ints = build(cholesky, groups, pairs)
    mine = ladder(ints, everyone, groups)
    return jnp.transpose(mine.reshape(-1, A_WIN, brows), (2, 1, 0))


def solution(mesh):
    in_specs = (P("pair", "grp", None), P("pair", "grp", None))
    return jax.shard_map(
        functools.partial(per_device, mesh.shape["grp"], mesh.shape["pair"]), mesh=mesh,
        in_specs=in_specs, out_specs=P("pair", None, "grp"), check_vma=False,
    )
```
